128 devices in a mesh: row: 8 (over x, y_hi), col: 16 (over y_lo, z, core).
Axes of the slice: x: 4, y: 4 (y_hi: 2, y_lo: 2; y = y_hi * 2 + y_lo), z: 4, core: 2. Of those that a mesh axis runs over, the one named last changes fastest.
Arguments:
- incoming: float32 [8, 16, 4, 128, 128], P('row', 'col'), may hold values from -6 to 6
- block_map: int32 [8, 16, 4], P('row', 'col'), may hold values from 0 to 511, as said below
- panel_row: float32 [2, 8, 128, 32, 16, 128], P(None, 'row', None, None, 'col'), may hold values from -0.125 to 0.125
- diag_inverse: float32 [1, 16, 128, 128], P(None, 'col'), may hold values from -1 to 2.5
Outputs:
- panel_solution: float32 [128, 1, 16, 128], P('row', None, 'col')
- trailing_rhs: float32 [128, 31, 16, 128], P('row', None, 'col')
The draws below stay inside these ranges and needn't reach their ends.
Inputs may be any that keep to these rules, and one draw needn't show every extreme that they name: block_map names every block index from 0 to 511 exactly once; the 4 blocks of one device lie in distinct grid columns, block b lying in grid column b mod 16.
All inputs are finite; a program needn't handle non-finite values.
Results may differ from the reference program's by a relative error of at most 0.00013.
Values sent between devices are 32-bit elements; how exact they have to be, the bound alone decides.
No kernel may reach another device: no remote copies, remote signals or barrier semaphores. Data moves between devices by JAX's collectives and lax.ppermute only.
A program may use at most 64 MiB of HBM per device.

```python
import jax
import jax.numpy as jnp
from jax import lax

NB = 128
PW = 2048
NRHS = 128
SRC_BLK = 4
ORDER = 65536
SLOTS = 32
NBLK = 512
PWB = 16
TR = 2
TC = 1
TSLOTS = 31
N_ROW = 8
N_COL = 16


def draw_block_map(key, part):
    first_key, second_key = jax.random.split(jax.random.fold_in(key, 11))
    row_keys = jax.random.split(first_key, N_ROW)
    offsets = jax.vmap(lambda subkey: jax.random.permutation(subkey, N_COL)[:SRC_BLK])(row_keys)
    devices_in = jnp.arange(N_COL, dtype=jnp.int32)
    column_of = (devices_in[None, :, None] + offsets[:, None, :]) % N_COL
    column_keys = jax.random.split(second_key, N_COL)
    orders = jax.vmap(lambda subkey: jax.random.permutation(subkey, SLOTS))(column_keys)
    entries = jnp.arange(N_ROW, dtype=jnp.int32)[:, None, None] * SRC_BLK + jnp.arange(SRC_BLK, dtype=jnp.int32)[None, None, :]
    entries = jnp.broadcast_to(entries, (N_ROW, N_COL, SRC_BLK))
    slot_of = orders[column_of, entries]
    return (slot_of * N_COL + column_of).astype(jnp.int32)


def draw_diag_inverse(key, part):
    first_key = jax.random.fold_in(jax.random.fold_in(key, 23), 0)
    identity = jnp.eye(NB, dtype=jnp.float32)
    noise = jnp.clip(jax.random.normal(first_key, (TC, N_COL, NB, NB), jnp.float32), -4.0, 4.0)
    diagonal = jnp.ones((TC, N_COL, NB, 1), jnp.float32)
    return diagonal * identity + 0.5 * noise / jnp.sqrt(jnp.float32(NB))


def block_scale(key, dims, cuts, smallest, top_value):
    def one(axis_at, blocks):
        heights = jax.random.uniform(jax.random.fold_in(jax.random.fold_in(key, 6), axis_at), (blocks,), jnp.float32, smallest / len(cuts), top_value / len(cuts))
        return jnp.repeat(jnp.exp(heights), dims[axis_at] // blocks).reshape((-1,) + (1,) * (len(dims) - axis_at - 1))

    factor_of = one(*cuts[0])
    for cut in cuts[1:]:
        factor_of = factor_of * one(*cut)
    return factor_of


def normal_values(stream_key, extent, spread, reach, cuts=(), kind=jnp.bfloat16):
    values = spread * jax.random.normal(stream_key, extent, jnp.float32)
    if cuts:
        values = values * block_scale(stream_key, extent, cuts, -0.22, 0.18)
    return jnp.clip(values, -reach, reach).astype(kind)


def setup_inputs(seed: int = 0) -> dict:
    streams_of = jax.random.split(jax.random.key(seed), 5)
    return {
        "incoming": normal_values(streams_of[0], (N_ROW, N_COL, SRC_BLK, NRHS, NB), 1.0, 6.0, ((0, 8), (1, 16)), jnp.float32),
        "block_map": draw_block_map(jax.random.fold_in(streams_of[4], 71), 0),
        "panel_row": normal_values(streams_of[2], (TR, N_ROW, NB, SLOTS, N_COL, NB), PW ** -0.5, 0.125, ((1, 8), (4, 16)), jnp.float32),
        "diag_inverse": draw_diag_inverse(jax.random.fold_in(streams_of[4], 71), 0),
    }


def reference(incoming, block_map, panel_row, diag_inverse):
    highest = lax.Precision.HIGHEST
    block_total = N_ROW * N_COL * SRC_BLK
    pieces = incoming.reshape(block_total, NRHS, NB)
    targets = block_map.reshape(block_total).astype(jnp.int32)
    placed = jnp.zeros((NBLK, NRHS, NB), jnp.float32).at[targets].set(pieces)
    rhs_rows = jnp.transpose(placed, (1, 0, 2)).reshape(NRHS, ORDER)
    upper_rows = panel_row.reshape(PW, ORDER)
    inverse = diag_inverse.reshape(PWB, NB, NB)
    solved = jnp.zeros((NRHS, PW), jnp.float32)
    for block_index in range(PWB):
        lower_edge = block_index * NB
        carried = jnp.dot(solved, upper_rows[:, lower_edge:lower_edge + NB], precision=highest, preferred_element_type=jnp.float32)
        residue = rhs_rows[:, lower_edge:lower_edge + NB] - carried
        solution_block = jnp.dot(residue, inverse[block_index].T, precision=highest, preferred_element_type=jnp.float32)
        solved = solved.at[:, lower_edge:lower_edge + NB].set(solution_block)
    update = jnp.dot(solved, upper_rows[:, PW:], precision=highest, preferred_element_type=jnp.float32)
    trailing = rhs_rows[:, PW:] - update
    return solved.reshape(NRHS, TC, N_COL, NB), trailing.reshape(NRHS, TSLOTS, N_COL, NB)
```

```python
import jax
import jax.numpy as jnp
from jax import lax
from jax.experimental import pallas as pl
from jax.experimental.pallas import tpu as pltpu
from jax.sharding import Mesh
from jax.sharding import PartitionSpec as P

HIGHEST = lax.Precision.HIGHEST
ROW = ("x", "yh")
COL = ("yl", "z", "core")
PLANE = ("z", "core")
BLOCK = 128


def rotated(array, axis, step):
    size = lax.axis_size(axis)
    return lax.ppermute(array, axis, [(i, (i + step) % size) for i in range(size)])


def around(array, axis):
    steps = range(1, lax.axis_size(axis))
    return jnp.stack([array] + [rotated(array, axis, step) for step in steps])


def to_everyone(array, axis):
    copies = jnp.broadcast_to(array, (lax.axis_size(axis), *array.shape))
    return lax.all_to_all(copies, axis, split_axis=0, concat_axis=0, tiled=True)


def split_bf16(value):
    high = value.astype(jnp.bfloat16)
    low = (value - high.astype(jnp.float32)).astype(jnp.bfloat16)
    return high, low


def solve_kernel(place_ref, start_ref, even_ref, odd_ref, out_ref):
    my_x, my_z, my_core = place_ref[0], place_ref[1], place_ref[2]
    blocks = start_ref.shape[0]
    rhs = start_ref.shape[1]

    def factor(j, i):
        dx = lax.rem(my_x - j // 2 + 4, 4)
        dz = lax.rem(my_z - i // 2 + 4, 4)
        dcore = lax.rem(my_core + i, 2)
        if j % 2 == 0:
            return even_ref[dcore, dz, dx]
        return odd_ref[dcore, dx, dz]

    rest = [start_ref[i] for i in range(blocks)]
    for j in range(blocks):
        done = rest[j]
        out_ref[j] = done
        high, low = split_bf16(done)
        both = jnp.concatenate([high, low], axis=0)
        for i in range(j + 1, blocks):
            w_high, w_low = split_bf16(factor(j, i))
            first = jnp.dot(both, w_high, preferred_element_type=jnp.float32)
            second = jnp.dot(high, w_low, preferred_element_type=jnp.float32)
            rest[i] = rest[i] - (first[:rhs] + first[rhs:] + second)


def solve_plane(place, start, even, odd):
    vmem = pl.BlockSpec(memory_space=pltpu.VMEM)
    return pl.pallas_call(
        solve_kernel,
        out_shape=jax.ShapeDtypeStruct(start.shape, jnp.float32),
        in_specs=[pl.BlockSpec(memory_space=pltpu.SMEM), vmem, vmem, vmem],
        out_specs=vmem,
        cost_estimate=pl.CostEstimate(flops=600_000_000, bytes_accessed=5_000_000, transcendentals=0),
    )(place, start, even, odd)


def per_device(incoming, block_map, panel_row, diag_inverse):
    my_x, my_yl, my_z, my_core = (lax.axis_index(a) for a in ("x", "yl", "z", "core"))
    my_yh = lax.axis_index("yh")
    my_col = lax.axis_index(COL)
    rows, cols = lax.axis_size(ROW), lax.axis_size(COL)
    plane = lax.axis_size(PLANE)
    sources = incoming.shape[2]
    share = BLOCK // rows
    slots = panel_row.shape[3]

    inverse = diag_inverse.reshape(BLOCK, BLOCK)
    upper = panel_row.reshape(2, BLOCK, slots, BLOCK)
    scaled = jnp.einsum("tpf,ef->tpe", upper[:, :, 0, :], inverse, precision=HIGHEST)
    mine = jnp.where(my_yl == 0, scaled[0], scaled[1])

    other = lax.ppermute(mine, "yh", [(0, 1), (1, 0)])
    even = jnp.where(my_yh == 0, mine, other)
    odd = jnp.where(my_yh == 0, other, mine)
    even = around(around(even, "x"), "z")
    odd = around(around(odd, "z"), "x")
    even = around(even, "core")
    odd = around(odd, "core")
    coupling = to_everyone(scaled[0], ROW)

    targets = block_map.reshape(sources)
    pieces = incoming.reshape(sources, rows, share, BLOCK)
    columns = jnp.arange(cols, dtype=jnp.int32)
    chosen = (targets[None, :] % cols) == columns[:, None]
    outgoing = jnp.zeros((rows, cols, share, BLOCK), jnp.float32)
    for u in range(sources):
        outgoing = jnp.where(chosen[None, :, u, None, None], pieces[u][:, None], outgoing)
    labels = jnp.max(jnp.where(chosen, targets[None, :] // cols, -1), axis=1).astype(jnp.float32)
    labels = jnp.broadcast_to(labels[None, :, None, None, None], (rows, cols, 1, 1, BLOCK))
    packed = jnp.concatenate([outgoing.reshape(rows, cols, share, 1, BLOCK), labels], axis=2)
    packed = packed.reshape(rows * cols, share + 1, 1, BLOCK)
    received = lax.all_to_all(packed, ROW + COL, 0, 0, tiled=True)
    slot_of = received[:, share, 0, 0].astype(jnp.int32)
    data = received[:, :share, 0, :]
    panel_rhs = jnp.sum(jnp.where((slot_of == 0)[:, None, None], data, 0.0), axis=0)
    matches = (slot_of[None, :] == jnp.arange(1, slots, dtype=jnp.int32)[:, None]).astype(jnp.float32)
    trailing_rhs = jnp.einsum("sq,qke->kse", matches, data, precision=HIGHEST)
    start = jnp.einsum("kf,ef->ke", panel_rhs, inverse, precision=HIGHEST)

    place = jnp.stack([my_x, my_z, my_core]).astype(jnp.int32)
    first = solve_plane(place, to_everyone(start, PLANE), even, odd)
    passed = lax.ppermute(first, "yl", [(0, 1)])
    carried = jnp.einsum("jkp,jpe->ke", passed, coupling, precision=HIGHEST)
    second = solve_plane(place, to_everyone(start - carried, PLANE), even, odd)
    solved = jnp.where(my_yl == 0, first, second)
    panel_solution = lax.dynamic_index_in_dim(solved, my_z * 2 + my_core, 0, keepdims=False)

    copies = jnp.broadcast_to(solved[:, None], (rows, 2, share, BLOCK))
    copies = copies.reshape(rows * 2, share, BLOCK)
    own_rows = lax.all_to_all(copies, ROW + ("yl",), 0, 0, tiled=True)
    own_rows = own_rows.reshape(rows, 2, share, BLOCK)
    partial = jnp.einsum("rtkp,tpse->rkse", own_rows, upper[:, :, 1:, :], precision=HIGHEST)
    parts = lax.all_to_all(partial, ROW, 0, 0, tiled=True)
    trailing = trailing_rhs - jnp.sum(parts, axis=0)
    return panel_solution[:, None, None, :], trailing[:, :, None, :]


def solution(mesh):
    fine = Mesh(mesh.devices.reshape(4, 2, 2, 4, 2), ("x", "yh", "yl", "z", "core"))
    in_specs = (
        P(ROW, COL, None, None, None),
        P(ROW, COL, None),
        P(None, ROW, None, None, COL, None),
        P(None, COL, None, None),
    )
    out_specs = (P(ROW, None, COL, None), P(ROW, None, COL, None))
    return jax.shard_map(
        per_device, mesh=fine, in_specs=in_specs, out_specs=out_specs, check_vma=False
    )
```

```python
import jax
import jax.numpy as jnp
from jax import lax
from jax.experimental import pallas as pl
from jax.experimental.pallas import tpu as pltpu
from jax.sharding import Mesh
from jax.sharding import PartitionSpec as P


HIGHEST = lax.Precision.HIGHEST
ROW = ("x", "yh")
COL = ("yl", "z", "core")
PLANE = ("z", "core")
BLOCK = 128
HALF = 8
VMEM = pl.BlockSpec(memory_space=pltpu.VMEM)
SMEM = pl.BlockSpec(memory_space=pltpu.SMEM)


def rotated(array, axis, step):
    size = lax.axis_size(axis)
    return lax.ppermute(array, axis, [(i, (i + step) % size) for i in range(size)])


def around(array, axis):
    steps = range(1, lax.axis_size(axis))
    return [array] + [rotated(array, axis, step) for step in steps]


def split_bf16(value):
    high = value.astype(jnp.bfloat16)
    low = (value - high.astype(jnp.float32)).astype(jnp.bfloat16)
    return high, low


def product(left, right, right_dim=0):
    l_high, l_low = left
    r_high, r_low = split_bf16(right)
    dims = (((1,), (right_dim,)), ((), ()))
    both = jnp.concatenate([l_high, l_low], axis=0)
    first = lax.dot_general(both, r_high, dims, preferred_element_type=jnp.float32)
    second = lax.dot_general(l_high, r_low, dims, preferred_element_type=jnp.float32)
    rows = l_high.shape[0]
    return first[:rows] + first[rows:] + second


def solve_blocks(place_ref, start, even_refs, odd_refs):
    my_x, my_z, my_core = place_ref[0], place_ref[1], place_ref[2]

    def factor(j, i):
        dx = lax.rem(my_x - j // 2 + 4, 4)
        dz = lax.rem(my_z - i // 2 + 4, 4)
        own_ref, other_ref = even_refs if j % 2 == 0 else odd_refs
        at = (dz, dx) if j % 2 == 0 else (dx, dz)
        return jnp.where(my_core == i % 2, own_ref[at], other_ref[at])

    rest = [product(split_bf16(start(i)), factor(i, i), 1) for i in range(HALF)]
    for j in range(HALF):
        done = split_bf16(rest[j])
        for i in range(j + 1, HALF):
            rest[i] = rest[i] - product(done, factor(j, i))
    return rest


def first_kernel(place_ref, start_ref, e0_ref, e1_ref, o0_ref, o1_ref, out_ref):
    solved = solve_blocks(
        place_ref, lambda i: start_ref[i], (e0_ref, e1_ref), (o0_ref, o1_ref)
    )
    for i in range(HALF):
        out_ref[i] = solved[i]


def coupling_kernel(place_ref, start_ref, passed_ref, x_ref, out_ref):
    my_x, my_z, my_core = place_ref[0], place_ref[1], place_ref[2]
    total = start_ref[my_z * 2 + my_core]
    for j in range(HALF):
        dx = lax.rem(my_x - j // 2 + 4, 4)
        total = total - product(split_bf16(passed_ref[j]), x_ref[dx, j % 2])
    out_ref[...] = total


def second_kernel(place_ref, start_ref, first_ref, e0_ref, e1_ref, o0_ref, o1_ref, out_ref):
    my_z, my_core = place_ref[1], place_ref[2]

    def start(i):
        return start_ref[lax.rem(my_z - i // 2 + 4, 4), lax.rem(my_core + i, 2)]

    solved = solve_blocks(place_ref, start, (e0_ref, e1_ref), (o0_ref, o1_ref))
    for i in range(HALF):
        block = jnp.where(place_ref[3] == 0, first_ref[i], solved[i])
        out_ref[i, 0] = block
        out_ref[i, 1] = block


def local_kernel(kernel, shape, *args):
    return pl.pallas_call(
        kernel,
        out_shape=jax.ShapeDtypeStruct(shape, jnp.float32),
        in_specs=[SMEM] + [VMEM] * (len(args) - 1),
        out_specs=VMEM,
        cost_estimate=pl.CostEstimate(flops=600_000_000, bytes_accessed=5_000_000, transcendentals=0),
    )(*args)


def per_device(incoming, block_map, panel_row, diag_inverse):
    my_x, my_yh, my_yl, my_z, my_core = (lax.axis_index(a) for a in ("x", "yh", "yl", "z", "core"))
    my_row = lax.axis_index(ROW)
    my_plane = lax.axis_index(PLANE)
    rows, cols = lax.axis_size(ROW), lax.axis_size(COL)
    sources = incoming.shape[2]
    share = BLOCK // rows
    slots = panel_row.shape[3]
    place = jnp.stack([my_x, my_z, my_core, my_yl]).astype(jnp.int32)

    targets = block_map.reshape(sources)
    blocks = incoming.reshape(sources, BLOCK, BLOCK)
    pieces = blocks.reshape(sources, rows, share, BLOCK).transpose(1, 0, 2, 3)
    labels = jnp.concatenate([targets, targets]).astype(jnp.float32)
    labels = jnp.broadcast_to(labels[None, :, None], (rows, 2 * sources, BLOCK))
    packed = jnp.concatenate([pieces.reshape(rows, sources * share, BLOCK), labels], axis=1)

    inverse = diag_inverse.reshape(BLOCK, BLOCK)
    upper = panel_row.reshape(2, BLOCK, slots, BLOCK)
    panel = upper[:, :, 0, :]
    scaled = jnp.einsum("tpf,ef->tpe", panel, inverse, precision=HIGHEST)
    mine = jnp.where(my_yl == 0, scaled[0], scaled[1])
    mine = jnp.where(my_row == my_plane, inverse, mine)

    pair = jnp.stack([mine, panel[0]])
    other = lax.ppermute(pair, "yh", [(0, 1), (1, 0)])
    even = jnp.where(my_yh == 0, pair, other)
    odd = jnp.where(my_yh == 0, other, pair)
    received = lax.all_to_all(packed, ROW, 0, 0, tiled=True)
    by_x = around(jnp.stack([even[0], even[1], odd[1]]), "x")
    by_z = around(odd[0], "z")
    coupling = jnp.stack([p[1:] for p in by_x])
    even = jnp.stack([p[0] for p in by_x])
    upper, even = lax.optimization_barrier((upper, even))
    even = jnp.stack(around(even, "z"))
    odd = jnp.stack(around(jnp.stack(by_z), "x"))

    data = received[:, : sources * share].reshape(rows, sources, share, BLOCK)
    label = received[:, sources * share : sources * share + sources, None, :]

    def belonging(half):
        wanted = (half * HALF + jnp.arange(HALF, dtype=jnp.int32)).astype(jnp.float32)
        return jnp.sum(
            jnp.where(label[None] == wanted[:, None, None, None, None], data[None], 0.0), axis=(1, 2)
        )

    start = belonging(my_yl) + rotated(belonging(1 - my_yl), "yl", 1)
    start = start + rotated(start, "core", 1)
    start = sum(around(start, "z"))

    even_other = rotated(even, "core", 1)
    odd_other = rotated(odd, "core", 1)
    factors = (even, even_other, odd, odd_other)

    chosen = (targets[None, :] % cols) == jnp.arange(cols, dtype=jnp.int32)[:, None]
    outgoing = jnp.zeros((cols, BLOCK, BLOCK), jnp.float32)
    for u in range(sources):
        outgoing = jnp.where(chosen[:, u, None, None], blocks[u][None], outgoing)
    slot_label = jnp.max(jnp.where(chosen, targets[None, :] // cols, -1), axis=1)
    slot_label = jnp.broadcast_to(slot_label.astype(jnp.float32)[:, None, None], (cols, 8, BLOCK))
    outgoing = jnp.concatenate([outgoing, slot_label], axis=1)

    shape = (HALF, share, BLOCK)
    first = local_kernel(first_kernel, shape, place, start, *factors)
    passed = lax.ppermute(first, "yl", [(0, 1)])
    arrived = lax.all_to_all(outgoing, COL, 0, 0, tiled=True)
    residual = local_kernel(
        coupling_kernel, (share, BLOCK), place, start, passed, coupling
    )
    residual = jnp.stack(around(jnp.stack(around(residual, "core")), "z"))
    copies = local_kernel(
        second_kernel, (HALF, 2, share, BLOCK), place, residual, first, *factors
    )
    copies, arrived = lax.optimization_barrier((copies, arrived))
    panel_solution = lax.dynamic_index_in_dim(copies[:, 0], my_plane, 0, keepdims=False)

    own_rows = lax.all_to_all(
        copies.reshape(rows * 2, share, BLOCK), ROW + ("yl",), 0, 0, tiled=True
    ).reshape(rows, 2, share, BLOCK)
    slot_of = arrived[:, BLOCK, 0].astype(jnp.int32)
    matches = (slot_of[None, :] == jnp.arange(1, slots, dtype=jnp.int32)[:, None]).astype(jnp.float32)
    held = arrived[:, :BLOCK].reshape(cols, rows, share, BLOCK)
    held = jnp.einsum("sq,qrke->rkse", matches, held, precision=HIGHEST)
    partial = held - jnp.einsum(
        "rtkp,tpse->rkse", own_rows, upper[:, :, 1:, :], precision=lax.Precision.HIGH
    )
    trailing = lax.dynamic_index_in_dim(partial, my_row, 0, keepdims=False)
    for step in range(1, rows):
        part = lax.dynamic_index_in_dim(partial, my_row ^ step, 0, keepdims=False)
        trailing = trailing + lax.ppermute(part, ROW, [(i, i ^ step) for i in range(rows)])
    return panel_solution[:, None, None, :], trailing[:, :, None, :]


def solution(mesh):
    fine = Mesh(mesh.devices.reshape(4, 2, 2, 4, 2), ("x", "yh", "yl", "z", "core"))
    in_specs = (
        P(ROW, COL, None, None, None),
        P(ROW, COL, None),
        P(None, ROW, None, None, COL, None),
        P(None, COL, None, None),
    )
    out_specs = (P(ROW, None, COL, None), P(ROW, None, COL, None))
    return jax.shard_map(per_device, mesh=fine, in_specs=in_specs, out_specs=out_specs, check_vma=False)
```

```python
import jax
import jax.numpy as jnp
from jax import lax
from jax.experimental import pallas as pl
from jax.experimental.pallas import tpu as pltpu
from jax.sharding import Mesh
from jax.sharding import PartitionSpec as P


HIGHEST = lax.Precision.HIGHEST
ROW = ("x", "yh")
COL = ("yl", "z", "core")
PLANE = ("z", "core")
BLOCK = 128
HALF = 8
VMEM = pl.BlockSpec(memory_space=pltpu.VMEM)
SMEM = pl.BlockSpec(memory_space=pltpu.SMEM)


def rotated(array, axis, step):
    size = lax.axis_size(axis)
    return lax.ppermute(array, axis, [(i, (i + step) % size) for i in range(size)])


def around(array, axis):
    steps = range(1, lax.axis_size(axis))
    return [array] + [rotated(array, axis, step) for step in steps]


def split_bf16(value):
    high = value.astype(jnp.bfloat16)
    low = (value - high.astype(jnp.float32)).astype(jnp.bfloat16)
    return high, low


def product(left, right, right_dim=0):
    l_high, l_low = left
    r_high, r_low = split_bf16(right)
    dims = (((1,), (right_dim,)), ((), ()))
    both = jnp.concatenate([l_high, l_low], axis=0)
    first = lax.dot_general(both, r_high, dims, preferred_element_type=jnp.float32)
    second = lax.dot_general(l_high, r_low, dims, preferred_element_type=jnp.float32)
    rows = l_high.shape[0]
    return first[:rows] + first[rows:] + second


def solve_blocks(place_ref, start, even_refs, odd_refs):
    my_x, my_z, my_core = place_ref[0], place_ref[1], place_ref[2]

    def factor(j, i):
        dx = lax.rem(my_x - j // 2 + 4, 4)
        dz = lax.rem(my_z - i // 2 + 4, 4)
        own_ref, other_ref = even_refs if j % 2 == 0 else odd_refs
        at = (dz, dx) if j % 2 == 0 else (dx, dz)
        return jnp.where(my_core == i % 2, own_ref[at], other_ref[at])

    rest = [product(split_bf16(start(i)), factor(i, i), 1) for i in range(HALF)]
    for j in range(HALF):
        done = split_bf16(rest[j])
        for i in range(j + 1, HALF):
            rest[i] = rest[i] - product(done, factor(j, i))
    return rest


def first_kernel(place_ref, start_ref, e0_ref, e1_ref, o0_ref, o1_ref, out_ref):
    solved = solve_blocks(
        place_ref, lambda i: start_ref[i], (e0_ref, e1_ref), (o0_ref, o1_ref)
    )
    for i in range(HALF):
        out_ref[i] = solved[i]


def coupling_kernel(place_ref, start_ref, passed_ref, x_ref, out_ref):
    my_x, my_z, my_core = place_ref[0], place_ref[1], place_ref[2]
    total = start_ref[my_z * 2 + my_core]
    for j in range(HALF):
        dx = lax.rem(my_x - j // 2 + 4, 4)
        total = total - product(split_bf16(passed_ref[j]), x_ref[dx, j % 2])
    out_ref[...] = total


def second_kernel(place_ref, start_ref, first_ref, e0_ref, e1_ref, o0_ref, o1_ref, out_ref):
    my_z, my_core = place_ref[1], place_ref[2]

    def start(i):
        return start_ref[lax.rem(my_z - i // 2 + 4, 4), lax.rem(my_core + i, 2)]

    solved = solve_blocks(place_ref, start, (e0_ref, e1_ref), (o0_ref, o1_ref))
    for i in range(HALF):
        block = jnp.where(place_ref[3] == 0, first_ref[i], solved[i])
        out_ref[i, 0] = block
        out_ref[i, 1] = block


def weights_kernel(after_ref, upper_ref, high_ref, low_ref):
    for s in range(upper_ref.shape[2]):
        high, low = split_bf16(upper_ref[:, :, s, :].reshape(2 * BLOCK, BLOCK))
        high_ref[s] = high
        low_ref[s] = low


def update_kernel(
    place_ref, slot_ref, rows_ref, held_ref, high_ref, low_ref,
    a_keep, a_send, b_keep, b_one, b_two, b_three, left_high, left_low,
):
    step = pl.program_id(0)
    count = high_ref.shape[0]
    last = pl.num_programs(0) - 1
    groups = [(yh, dx) for yh in range(2) for dx in range(4)]
    share = BLOCK // len(groups)

    def group_row(yh, dx):
        return lax.rem(place_ref[0] + dx, 4) * 2 + lax.rem(place_ref[4] + yh, 2)

    @pl.when(step == 0)
    def _():
        for g, (yh, dx) in enumerate(groups):
            for t in range(2):
                high, low = split_bf16(-rows_ref[group_row(yh, dx), t])
                at = (pl.ds(g * share, share), pl.ds(t * BLOCK, BLOCK))
                left_high[at] = high
                left_low[at] = low

    def put(slot, values, add):
        @pl.when(slot < 16)
        def _():
            for g, (yh, dx) in enumerate(groups):
                ref = (a_keep, a_send)[yh].at[dx, jnp.maximum(slot - 1, 0)]
                ref[...] = values(g) + ref[...] if add else values(g)

        @pl.when(slot >= 16)
        def _():
            for g, (yh, dx) in enumerate(groups):
                ref = (b_keep, b_one, b_two, b_three)[dx].at[yh, jnp.maximum(slot - 16, 0)]
                ref[...] = values(g) + ref[...] if add else values(g)

    for i in range(count):
        both = jnp.concatenate([left_high[...], left_low[...]], axis=0)
        first = jnp.dot(both, high_ref[i], preferred_element_type=jnp.float32)
        second = jnp.dot(left_high[...], low_ref[i], preferred_element_type=jnp.float32)
        total = first[:BLOCK] + first[BLOCK:] + second
        put(step * count + i, lambda g: total[g * share : (g + 1) * share], False)

    @pl.when(step == last)
    def _():
        def join(q, carry):
            def values(g):
                row = group_row(*groups[g]) * share
                return held_ref[q, pl.ds(pl.multiple_of(row, share), share), :]

            @pl.when(slot_ref[q] >= 1)
            def _():
                put(slot_ref[q], values, True)

            return carry

        lax.fori_loop(0, held_ref.shape[0], join, 0)


def local_kernel(kernel, shape, *args):
    return pl.pallas_call(
        kernel,
        out_shape=jax.ShapeDtypeStruct(shape, jnp.float32),
        in_specs=[SMEM] + [VMEM] * (len(args) - 1),
        out_specs=VMEM,
        cost_estimate=pl.CostEstimate(flops=600_000_000, bytes_accessed=5_000_000, transcendentals=0),
    )(*args)


def split_weights(after, upper):
    slots, step = upper.shape[2], 8
    shape = jax.ShapeDtypeStruct((slots, 2 * BLOCK, BLOCK), jnp.bfloat16)
    spec = pl.BlockSpec((step, 2 * BLOCK, BLOCK), lambda i: (i, 0, 0))
    return pl.pallas_call(
        weights_kernel,
        out_shape=(shape, shape),
        grid=(slots // step,),
        in_specs=[
            pl.BlockSpec((8, BLOCK), lambda i: (0, 0)),
            pl.BlockSpec((2, BLOCK, step, BLOCK), lambda i: (0, 0, i, 0)),
        ],
        out_specs=(spec, spec),
        cost_estimate=pl.CostEstimate(flops=600_000_000, bytes_accessed=8_000_000, transcendentals=0),
    )(after, upper)


def update(place, slot_of, own_rows, arrived, high, low):
    slots, step = high.shape[0], 8
    share = own_rows.shape[2]
    spec = pl.BlockSpec((step, 2 * BLOCK, BLOCK), lambda i: (i, 0, 0))
    shapes = [(4, 15, share, BLOCK)] * 2 + [(2, 16, share, BLOCK)] * 4
    return pl.pallas_call(
        update_kernel,
        out_shape=tuple(jax.ShapeDtypeStruct(shape, jnp.float32) for shape in shapes),
        grid=(slots // step,),
        in_specs=[SMEM, SMEM, VMEM, VMEM, spec, spec],
        out_specs=(VMEM,) * 6,
        scratch_shapes=[pltpu.VMEM((BLOCK, 2 * BLOCK), jnp.bfloat16)] * 2,
        cost_estimate=pl.CostEstimate(flops=900_000_000, bytes_accessed=8_000_000, transcendentals=0),
    )(place, slot_of, own_rows, arrived, high, low)


def per_device(incoming, block_map, panel_row, diag_inverse):
    my_x, my_yh, my_yl, my_z, my_core = (lax.axis_index(a) for a in ("x", "yh", "yl", "z", "core"))
    my_row = lax.axis_index(ROW)
    my_plane = lax.axis_index(PLANE)
    rows, cols = lax.axis_size(ROW), lax.axis_size(COL)
    sources = incoming.shape[2]
    share = BLOCK // rows
    slots = panel_row.shape[3]
    place = jnp.stack([my_x, my_z, my_core, my_yl, my_yh]).astype(jnp.int32)

    targets = block_map.reshape(sources)
    blocks = incoming.reshape(sources, BLOCK, BLOCK)
    pieces = blocks.reshape(sources, rows, share, BLOCK).transpose(1, 0, 2, 3)
    labels = jnp.concatenate([targets, targets]).astype(jnp.float32)
    labels = jnp.broadcast_to(labels[None, :, None], (rows, 2 * sources, BLOCK))
    packed = jnp.concatenate([pieces.reshape(rows, sources * share, BLOCK), labels], axis=1)

    inverse = diag_inverse.reshape(BLOCK, BLOCK)
    upper = panel_row.reshape(2, BLOCK, slots, BLOCK)
    panel = upper[:, :, 0, :]
    scaled = jnp.einsum("tpf,ef->tpe", panel, inverse, precision=HIGHEST)
    mine = jnp.where(my_yl == 0, scaled[0], scaled[1])
    mine = jnp.where(my_row == my_plane, inverse, mine)

    pair = jnp.stack([mine, panel[0]])
    other = lax.ppermute(pair, "yh", [(0, 1), (1, 0)])
    even = jnp.where(my_yh == 0, pair, other)
    odd = jnp.where(my_yh == 0, other, pair)
    received = lax.all_to_all(packed, ROW, 0, 0, tiled=True)
    by_x = around(jnp.stack([even[0], even[1], odd[1]]), "x")
    by_z = around(odd[0], "z")
    coupling = jnp.stack([p[1:] for p in by_x])
    even = jnp.stack([p[0] for p in by_x])
    weights = split_weights(by_x[1][0, :8], upper)
    even = jnp.stack(around(even, "z"))
    odd = jnp.stack(around(jnp.stack(by_z), "x"))

    data = received[:, : sources * share].reshape(rows, sources, share, BLOCK)
    label = received[:, sources * share : sources * share + sources, None, :]

    def belonging(half):
        wanted = (half * HALF + jnp.arange(HALF, dtype=jnp.int32)).astype(jnp.float32)
        return jnp.sum(
            jnp.where(label[None] == wanted[:, None, None, None, None], data[None], 0.0), axis=(1, 2)
        )

    start = belonging(my_yl) + rotated(belonging(1 - my_yl), "yl", 1)
    start = start + rotated(start, "core", 1)
    start = sum(around(start, "z"))

    chosen = (targets[None, :] % cols) == jnp.arange(cols, dtype=jnp.int32)[:, None]
    outgoing = jnp.zeros((cols, BLOCK, BLOCK), jnp.float32)
    for u in range(sources):
        outgoing = jnp.where(chosen[:, u, None, None], blocks[u][None], outgoing)
    slot_label = jnp.max(jnp.where(chosen, targets[None, :] // cols, -1), axis=1)
    slot_label = jnp.broadcast_to(slot_label.astype(jnp.float32)[:, None, None], (cols, 8, BLOCK))
    outgoing = jnp.concatenate([outgoing, slot_label], axis=1)

    even, odd, start, coupling, outgoing = lax.optimization_barrier(
        (even, odd, start, coupling, outgoing)
    )
    factors = (even, rotated(even, "core", 1), odd, rotated(odd, "core", 1))

    shape = (HALF, share, BLOCK)
    first = local_kernel(first_kernel, shape, place, start, *factors)
    passed = lax.ppermute(first, "yl", [(0, 1)])
    arrived = lax.all_to_all(outgoing, COL, 0, 0, tiled=True)
    residual = local_kernel(
        coupling_kernel, (share, BLOCK), place, start, passed, coupling
    )
    residual = jnp.stack(around(jnp.stack(around(residual, "core")), "z"))
    copies = local_kernel(second_kernel, (HALF, 2, share, BLOCK), place, residual, first, *factors)
    copies, arrived = lax.optimization_barrier((copies, arrived))
    panel_solution = lax.dynamic_index_in_dim(copies[:, 0], my_plane, 0, keepdims=False)

    own_rows = lax.all_to_all(
        copies.reshape(rows * 2, share, BLOCK), ROW + ("yl",), 0, 0, tiled=True
    ).reshape(rows, 2, share, BLOCK)
    slot_of = arrived[:, BLOCK, 0].astype(jnp.int32)
    a_keep, a_send, b_keep, *b_sends = update(place, slot_of, own_rows, arrived, *weights)
    a_part = a_keep + rotated(a_send, "yh", 1)
    b_part = b_keep
    for step, b_send in zip((1, 2, 3), b_sends):
        b_part = b_part + rotated(b_send, "x", step)
    b_part = b_part[0] + rotated(b_part[1], "yh", 1)
    a_part = a_part[0] + sum(rotated(a_part[step], "x", step) for step in (1, 2, 3))
    trailing = jnp.concatenate([a_part, b_part], axis=0).transpose(1, 0, 2)
    return panel_solution[:, None, None, :], trailing[:, :, None, :]


def solution(mesh):
    fine = Mesh(mesh.devices.reshape(4, 2, 2, 4, 2), ("x", "yh", "yl", "z", "core"))
    in_specs = (
        P(ROW, COL, None, None, None),
        P(ROW, COL, None),
        P(None, ROW, None, None, COL, None),
        P(None, COL, None, None),
    )
    out_specs = (P(ROW, None, COL, None), P(ROW, None, COL, None))
    return jax.shard_map(
        per_device, mesh=fine, in_specs=in_specs, out_specs=out_specs, check_vma=False
    )
```

```python
import jax
import jax.numpy as jnp
from jax import lax
from jax.experimental import pallas as pl
from jax.experimental.layout import Layout, with_layout_constraint
from jax.experimental.pallas import tpu as pltpu
from jax.sharding import Mesh
from jax.sharding import PartitionSpec as P


HIGHEST = lax.Precision.HIGHEST
ROW = ("x", "yh")
COL = ("yl", "z", "core")
PLANE = ("z", "core")
BLOCK = 128
HALF = 8
VMEM = pl.BlockSpec(memory_space=pltpu.VMEM)
SMEM = pl.BlockSpec(memory_space=pltpu.SMEM)


def rotated(array, axis, step):
    size = lax.axis_size(axis)
    return lax.ppermute(array, axis, [(i, (i + step) % size) for i in range(size)])


def around(array, axis):
    steps = range(1, lax.axis_size(axis))
    return [array] + [rotated(array, axis, step) for step in steps]


def split_bf16(value):
    high = value.astype(jnp.bfloat16)
    low = (value - high.astype(jnp.float32)).astype(jnp.bfloat16)
    return high, low


def product(left, right, right_dim=0):
    l_high, l_low = left
    r_high, r_low = split_bf16(right)
    dims = (((1,), (right_dim,)), ((), ()))
    both = jnp.concatenate([l_high, l_low], axis=0)
    first = lax.dot_general(both, r_high, dims, preferred_element_type=jnp.float32)
    second = lax.dot_general(l_high, r_low, dims, preferred_element_type=jnp.float32)
    rows = l_high.shape[0]
    return first[:rows] + first[rows:] + second


def solve_blocks(place_ref, start, even_refs, odd_refs):
    my_x, my_z, my_core = place_ref[0], place_ref[1], place_ref[2]

    def factor(j, i):
        dx = lax.rem(my_x - j // 2 + 4, 4)
        dz = lax.rem(my_z - i // 2 + 4, 4)
        own_ref, other_ref = even_refs if j % 2 == 0 else odd_refs
        at = (dz, dx) if j % 2 == 0 else (dx, dz)
        return jnp.where(my_core == i % 2, own_ref[at], other_ref[at])

    rest = [product(split_bf16(start(i)), factor(i, i), 1) for i in range(HALF)]
    for j in range(HALF):
        done = split_bf16(rest[j])
        for i in range(j + 1, HALF):
            rest[i] = rest[i] - product(done, factor(j, i))
    return rest


def first_kernel(place_ref, start_ref, e0_ref, e1_ref, o0_ref, o1_ref, out_ref):
    solved = solve_blocks(
        place_ref, lambda i: start_ref[i], (e0_ref, e1_ref), (o0_ref, o1_ref)
    )
    for i in range(HALF):
        out_ref[i] = solved[i]


def coupling_kernel(place_ref, start_ref, passed_ref, x_ref, out_ref):
    my_x, my_z, my_core = place_ref[0], place_ref[1], place_ref[2]
    total = start_ref[my_z * 2 + my_core]
    for j in range(HALF):
        dx = lax.rem(my_x - j // 2 + 4, 4)
        total = total - product(split_bf16(passed_ref[j]), x_ref[dx, j % 2])
    out_ref[...] = total


def second_kernel(place_ref, start_ref, first_ref, e0_ref, e1_ref, o0_ref, o1_ref, out_ref):
    my_z, my_core = place_ref[1], place_ref[2]

    def start(i):
        return start_ref[lax.rem(my_z - i // 2 + 4, 4), lax.rem(my_core + i, 2)]

    solved = solve_blocks(place_ref, start, (e0_ref, e1_ref), (o0_ref, o1_ref))
    for i in range(HALF):
        block = jnp.where(place_ref[3] == 0, first_ref[i], solved[i])
        out_ref[i, 0] = block
        out_ref[i, 1] = block


def update_kernel(
    place_ref, slot_ref, rows_ref, held_ref, factor_ref,
    a_keep, a_send, b_keep, b_one, b_two, b_three, left_high, left_low,
):
    step = pl.program_id(0)
    count = factor_ref.shape[1]
    last = pl.num_programs(0) - 1
    groups = [(yh, dx) for yh in range(2) for dx in range(4)]
    share = BLOCK // len(groups)

    def group_row(yh, dx):
        return lax.rem(place_ref[0] + dx, 4) * 2 + lax.rem(place_ref[4] + yh, 2)

    @pl.when(step == 0)
    def _():
        for g, (yh, dx) in enumerate(groups):
            for t in range(2):
                high, low = split_bf16(-rows_ref[group_row(yh, dx), t])
                at = (pl.ds(g * share, share), pl.ds(t * BLOCK, BLOCK))
                left_high[at] = high
                left_low[at] = low

    def put(slot, values, add):
        @pl.when(slot < 16)
        def _():
            for g, (yh, dx) in enumerate(groups):
                ref = (a_keep, a_send)[yh].at[dx, jnp.maximum(slot - 1, 0)]
                ref[...] = values(g) + ref[...] if add else values(g)

        @pl.when(slot >= 16)
        def _():
            for g, (yh, dx) in enumerate(groups):
                ref = (b_keep, b_one, b_two, b_three)[dx].at[yh, jnp.maximum(slot - 16, 0)]
                ref[...] = values(g) + ref[...] if add else values(g)

    for i in range(0, count, 2):
        halves = [jnp.concatenate([factor_ref[t, i], factor_ref[t, i + 1]], axis=1) for t in range(2)]
        high, low = split_bf16(jnp.concatenate(halves, axis=0))
        both = jnp.concatenate([left_high[...], left_low[...]], axis=0)
        first = jnp.dot(both, high, preferred_element_type=jnp.float32)
        second = jnp.dot(left_high[...], low, preferred_element_type=jnp.float32)
        total = first[:BLOCK] + first[BLOCK:] + second
        for k in range(2):
            part = total[:, k * BLOCK : (k + 1) * BLOCK]
            put(step * count + i + k, lambda g: part[g * share : (g + 1) * share], False)

    @pl.when(step == last)
    def _():
        def join(q, carry):
            def values(g):
                row = group_row(*groups[g]) * share
                return held_ref[q, pl.ds(pl.multiple_of(row, share), share), :]

            @pl.when(slot_ref[q] >= 1)
            def _():
                put(slot_ref[q], values, True)

            return carry

        lax.fori_loop(0, held_ref.shape[0], join, 0)


def local_kernel(kernel, shape, *args):
    return pl.pallas_call(
        kernel,
        out_shape=jax.ShapeDtypeStruct(shape, jnp.float32),
        in_specs=[SMEM] + [VMEM] * (len(args) - 1),
        out_specs=VMEM,
        cost_estimate=pl.CostEstimate(flops=600_000_000, bytes_accessed=5_000_000, transcendentals=0),
    )(*args)


def update(place, slot_of, own_rows, arrived, factor):
    slots, step = factor.shape[1], 8
    share = own_rows.shape[2]
    spec = pl.BlockSpec((2, step, BLOCK, BLOCK), lambda i: (0, i, 0, 0))
    shapes = [(4, 15, share, BLOCK)] * 2 + [(2, 16, share, BLOCK)] * 4
    return pl.pallas_call(
        update_kernel,
        out_shape=tuple(jax.ShapeDtypeStruct(shape, jnp.float32) for shape in shapes),
        grid=(slots // step,),
        in_specs=[SMEM, SMEM, VMEM, VMEM, spec],
        out_specs=(VMEM,) * 6,
        scratch_shapes=[pltpu.VMEM((BLOCK, 2 * BLOCK), jnp.bfloat16)] * 2,
        cost_estimate=pl.CostEstimate(flops=900_000_000, bytes_accessed=8_000_000, transcendentals=0),
    )(place, slot_of, own_rows, arrived, factor)


def per_device(incoming, block_map, panel_row, diag_inverse):
    my_x, my_yh, my_yl, my_z, my_core = (lax.axis_index(a) for a in ("x", "yh", "yl", "z", "core"))
    my_row = lax.axis_index(ROW)
    my_plane = lax.axis_index(PLANE)
    rows, cols = lax.axis_size(ROW), lax.axis_size(COL)
    sources = incoming.shape[2]
    share = BLOCK // rows
    slots = panel_row.shape[3]
    place = jnp.stack([my_x, my_z, my_core, my_yl, my_yh]).astype(jnp.int32)

    targets = block_map.reshape(sources)
    blocks = incoming.reshape(sources, BLOCK, BLOCK)
    pieces = blocks.reshape(sources, rows, share, BLOCK).transpose(1, 0, 2, 3)
    labels = jnp.concatenate([targets, targets]).astype(jnp.float32)
    labels = jnp.broadcast_to(labels[None, :, None], (rows, 2 * sources, BLOCK))
    packed = jnp.concatenate([pieces.reshape(rows, sources * share, BLOCK), labels], axis=1)

    inverse = diag_inverse.reshape(BLOCK, BLOCK)
    upper = panel_row.reshape(2, BLOCK, slots, BLOCK)
    panel = upper[:, :, 0, :]
    scaled = jnp.einsum("tpf,ef->tpe", panel, inverse, precision=HIGHEST)
    mine = jnp.where(my_yl == 0, scaled[0], scaled[1])
    mine = jnp.where(my_row == my_plane, inverse, mine)

    pair = jnp.stack([mine, panel[0]])
    other = lax.ppermute(pair, "yh", [(0, 1), (1, 0)])
    even = jnp.where(my_yh == 0, pair, other)
    odd = jnp.where(my_yh == 0, other, pair)
    received = lax.all_to_all(packed, ROW, 0, 0, tiled=True)
    by_x = around(jnp.stack([even[0], even[1], odd[1]]), "x")
    by_z = around(odd[0], "z")
    coupling = jnp.stack([p[1:] for p in by_x])
    even = jnp.stack([p[0] for p in by_x])
    upper, even = lax.optimization_barrier((upper, even))
    upper = with_layout_constraint(upper, Layout(major_to_minor=(0, 1, 2, 3)))
    factor = upper.transpose(0, 2, 1, 3)
    even = jnp.stack(around(even, "z"))
    odd = jnp.stack(around(jnp.stack(by_z), "x"))

    data = received[:, : sources * share].reshape(rows, sources, share, BLOCK)
    label = received[:, sources * share : sources * share + sources, None, :]

    def belonging(half):
        wanted = (half * HALF + jnp.arange(HALF, dtype=jnp.int32)).astype(jnp.float32)
        return jnp.sum(
            jnp.where(label[None] == wanted[:, None, None, None, None], data[None], 0.0), axis=(1, 2)
        )

    start = belonging(my_yl) + rotated(belonging(1 - my_yl), "yl", 1)
    start = start + rotated(start, "core", 1)
    start = sum(around(start, "z"))

    chosen = (targets[None, :] % cols) == jnp.arange(cols, dtype=jnp.int32)[:, None]
    outgoing = jnp.zeros((cols, BLOCK, BLOCK), jnp.float32)
    for u in range(sources):
        outgoing = jnp.where(chosen[:, u, None, None], blocks[u][None], outgoing)
    slot_label = jnp.max(jnp.where(chosen, targets[None, :] // cols, -1), axis=1)
    slot_label = jnp.broadcast_to(slot_label.astype(jnp.float32)[:, None, None], (cols, 8, BLOCK))
    outgoing = jnp.concatenate([outgoing, slot_label], axis=1)

    even, odd, start, coupling, outgoing = lax.optimization_barrier(
        (even, odd, start, coupling, outgoing)
    )
    factors = (even, rotated(even, "core", 1), odd, rotated(odd, "core", 1))

    shape = (HALF, share, BLOCK)
    first = local_kernel(first_kernel, shape, place, start, *factors)
    passed = lax.ppermute(first, "yl", [(0, 1)])
    arrived = lax.all_to_all(outgoing, COL, 0, 0, tiled=True)
    residual = local_kernel(
        coupling_kernel, (share, BLOCK), place, start, passed, coupling
    )
    residual = jnp.stack(around(jnp.stack(around(residual, "core")), "z"))
    copies = local_kernel(second_kernel, (HALF, 2, share, BLOCK), place, residual, first, *factors)
    copies, arrived = lax.optimization_barrier((copies, arrived))
    panel_solution = lax.dynamic_index_in_dim(copies[:, 0], my_plane, 0, keepdims=False)

    own_rows = lax.all_to_all(
        copies.reshape(rows * 2, share, BLOCK), ROW + ("yl",), 0, 0, tiled=True
    ).reshape(rows, 2, share, BLOCK)
    slot_of = arrived[:, BLOCK, 0].astype(jnp.int32)
    a_keep, a_send, b_keep, *b_sends = update(place, slot_of, own_rows, arrived, factor)
    a_part = a_keep + rotated(a_send, "yh", 1)
    b_part = b_keep
    for step, b_send in zip((1, 2, 3), b_sends):
        b_part = b_part + rotated(b_send, "x", step)
    b_part = b_part[0] + rotated(b_part[1], "yh", 1)
    a_part = a_part[0] + sum(rotated(a_part[step], "x", step) for step in (1, 2, 3))
    trailing = jnp.concatenate([a_part, b_part], axis=0).transpose(1, 0, 2)
    return panel_solution[:, None, None, :], trailing[:, :, None, :]


def solution(mesh):
    fine = Mesh(mesh.devices.reshape(4, 2, 2, 4, 2), ("x", "yh", "yl", "z", "core"))
    in_specs = (
        P(ROW, COL, None, None, None),
        P(ROW, COL, None),
        P(None, ROW, None, None, COL, None),
        P(None, COL, None, None),
    )
    out_specs = (P(ROW, None, COL, None), P(ROW, None, COL, None))
    return jax.shard_map(
        per_device, mesh=fine, in_specs=in_specs, out_specs=out_specs, check_vma=False
    )
```

```python
import jax
import jax.numpy as jnp
from jax import lax
from jax.experimental import pallas as pl
from jax.experimental.layout import Layout, with_layout_constraint
from jax.experimental.pallas import tpu as pltpu
from jax.sharding import Mesh
from jax.sharding import PartitionSpec as P


HIGHEST = lax.Precision.HIGHEST
ROW = ("x", "yh")
COL = ("yl", "z", "core")
PLANE = ("z", "core")
BLOCK = 128
HALF = 8
VMEM = pl.BlockSpec(memory_space=pltpu.VMEM)
SMEM = pl.BlockSpec(memory_space=pltpu.SMEM)


def rotated(array, axis, step):
    size = lax.axis_size(axis)
    return lax.ppermute(array, axis, [(i, (i + step) % size) for i in range(size)])


def around(array, axis):
    steps = range(1, lax.axis_size(axis))
    return [array] + [rotated(array, axis, step) for step in steps]


def split_bf16(value):
    high = value.astype(jnp.bfloat16)
    low = (value - high.astype(jnp.float32)).astype(jnp.bfloat16)
    return high, low


def product(left, right, right_dim=0):
    l_high, l_low = left
    r_high, r_low = split_bf16(right)
    dims = (((1,), (right_dim,)), ((), ()))
    both = jnp.concatenate([l_high, l_low], axis=0)
    first = lax.dot_general(both, r_high, dims, preferred_element_type=jnp.float32)
    second = lax.dot_general(l_high, r_low, dims, preferred_element_type=jnp.float32)
    rows = l_high.shape[0]
    return first[:rows] + first[rows:] + second


def solve_blocks(place_ref, start, even_refs, odd_refs):
    my_x, my_z, my_core = place_ref[0], place_ref[1], place_ref[2]

    def factor(j, i):
        dx = lax.rem(my_x - j // 2 + 4, 4)
        dz = lax.rem(my_z - i // 2 + 4, 4)
        own_ref, other_ref = even_refs if j % 2 == 0 else odd_refs
        at = (dz, dx) if j % 2 == 0 else (dx, dz)
        return jnp.where(my_core == i % 2, own_ref[at], other_ref[at])

    rest = [product(split_bf16(start(i)), factor(i, i), 1) for i in range(HALF)]
    for j in range(HALF):
        done = split_bf16(rest[j])
        for i in range(j + 1, HALF):
            rest[i] = rest[i] - product(done, factor(j, i))
    return rest


def first_kernel(place_ref, start_ref, e0_ref, e1_ref, o0_ref, o1_ref, out_ref):
    solved = solve_blocks(
        place_ref, lambda i: start_ref[i], (e0_ref, e1_ref), (o0_ref, o1_ref)
    )
    for i in range(HALF):
        out_ref[i] = solved[i]


def coupling_kernel(place_ref, start_ref, passed_ref, x_ref, out_ref):
    my_x, my_z, my_core = place_ref[0], place_ref[1], place_ref[2]
    left = jnp.concatenate([passed_ref[j] for j in range(HALF)], axis=1)
    right = [x_ref[lax.rem(my_x - j // 2 + 4, 4), j % 2] for j in range(HALF)]
    carried = product(split_bf16(left), jnp.concatenate(right, axis=0))
    out_ref[...] = start_ref[my_z * 2 + my_core] - carried


def second_kernel(place_ref, start_ref, first_ref, e0_ref, e1_ref, o0_ref, o1_ref, out_ref):
    my_z, my_core = place_ref[1], place_ref[2]

    def start(i):
        return start_ref[lax.rem(my_z - i // 2 + 4, 4), lax.rem(my_core + i, 2)]

    solved = solve_blocks(place_ref, start, (e0_ref, e1_ref), (o0_ref, o1_ref))
    for i in range(HALF):
        block = jnp.where(place_ref[3] == 0, first_ref[i], solved[i])
        out_ref[i, 0] = block
        out_ref[i, 1] = block


def update_kernel(
    place_ref, rows_ref, factor_ref, a_keep, a_send, b_keep, b_one, b_two, b_three, left_high, left_low
):
    step = pl.program_id(0)
    count = factor_ref.shape[1]
    groups = [(yh, dx) for yh in range(2) for dx in range(4)]
    share = BLOCK // len(groups)

    @pl.when(step == 0)
    def _():
        for g, (yh, dx) in enumerate(groups):
            row = lax.rem(place_ref[0] + dx, 4) * 2 + lax.rem(place_ref[4] + yh, 2)
            for t in range(2):
                high, low = split_bf16(-rows_ref[row, t])
                at = (pl.ds(g * share, share), pl.ds(t * BLOCK, BLOCK))
                left_high[at] = high
                left_low[at] = low

    def fill(target):
        both = jnp.concatenate([left_high[...], left_low[...]], axis=0)
        for i in range(0, count, 2):
            halves = [
                jnp.concatenate([factor_ref[t, i], factor_ref[t, i + 1]], axis=1) for t in range(2)
            ]
            high, low = split_bf16(jnp.concatenate(halves, axis=0))
            first = jnp.dot(both, high, preferred_element_type=jnp.float32)
            second = jnp.dot(left_high[...], low, preferred_element_type=jnp.float32)
            total = first[:BLOCK] + first[BLOCK:] + second
            for k in range(2):
                for g, (yh, dx) in enumerate(groups):
                    target(i + k, yh, dx, total[g * share : (g + 1) * share, k * BLOCK : (k + 1) * BLOCK])

    def fill_a(slot, yh, dx, values):
        if slot > 0:
            (a_keep, a_send)[yh][dx, slot - 1] = values

    def fill_b(slot, yh, dx, values):
        (b_keep, b_one, b_two, b_three)[dx][yh, slot] = values

    pl.when(step == 0)(lambda: fill(fill_a))
    pl.when(step == 1)(lambda: fill(fill_b))


def place_kernel(slot_ref, arrived_ref, out_ref):
    spare = out_ref.shape[0] - 1
    share = out_ref.shape[1]
    for q in range(slot_ref.shape[0]):
        slot = slot_ref[q]
        rows = pl.ds(q % 8 * share, share)
        out_ref[jnp.where(slot < 0, spare, slot)] = arrived_ref[q // 8, rows, :]


def local_kernel(kernel, shape, *args):
    return pl.pallas_call(
        kernel,
        out_shape=jax.ShapeDtypeStruct(shape, jnp.float32),
        in_specs=[SMEM] + [VMEM] * (len(args) - 1),
        out_specs=VMEM,
        cost_estimate=pl.CostEstimate(flops=600_000_000, bytes_accessed=5_000_000, transcendentals=0),
    )(*args)


def update(place, own_rows, factor):
    slots, step = factor.shape[1], 16
    share = own_rows.shape[2]
    spec = pl.BlockSpec((2, step, BLOCK, BLOCK), lambda i: (0, i, 0, 0))
    shapes = [(4, 15, share, BLOCK)] * 2 + [(2, 16, share, BLOCK)] * 4
    return pl.pallas_call(
        update_kernel,
        out_shape=tuple(jax.ShapeDtypeStruct(shape, jnp.float32) for shape in shapes),
        grid=(slots // step,),
        in_specs=[SMEM, VMEM, spec],
        out_specs=(VMEM,) * 6,
        scratch_shapes=[pltpu.VMEM((BLOCK, 2 * BLOCK), jnp.bfloat16)] * 2,
        cost_estimate=pl.CostEstimate(flops=900_000_000, bytes_accessed=8_000_000, transcendentals=0),
    )(place, own_rows, factor)


def per_device(incoming, block_map, panel_row, diag_inverse):
    my_x, my_yh, my_yl, my_z, my_core = (lax.axis_index(a) for a in ("x", "yh", "yl", "z", "core"))
    my_row = lax.axis_index(ROW)
    my_plane = lax.axis_index(PLANE)
    rows, cols = lax.axis_size(ROW), lax.axis_size(COL)
    sources = incoming.shape[2]
    share = BLOCK // rows
    slots = panel_row.shape[3]
    place = jnp.stack([my_x, my_z, my_core, my_yl, my_yh]).astype(jnp.int32)

    targets = block_map.reshape(sources)
    blocks = incoming.reshape(sources, BLOCK, BLOCK)
    pieces = blocks.reshape(sources, rows, share, BLOCK).transpose(1, 0, 2, 3)
    labels = jnp.concatenate([targets, targets]).astype(jnp.float32)
    labels = jnp.broadcast_to(labels[None, :, None], (rows, 2 * sources, BLOCK))
    packed = jnp.concatenate([pieces.reshape(rows, sources * share, BLOCK), labels], axis=1)

    inverse = diag_inverse.reshape(BLOCK, BLOCK)
    upper = panel_row.reshape(2, BLOCK, slots, BLOCK)
    panel = upper[:, :, 0, :]
    scaled = jnp.einsum("tpf,ef->tpe", panel, inverse, precision=HIGHEST)
    mine = jnp.where(my_yl == 0, scaled[0], scaled[1])
    mine = jnp.where(my_row == my_plane, inverse, mine)

    pair = jnp.stack([mine, panel[0]])
    other = lax.ppermute(pair, "yh", [(0, 1), (1, 0)])
    even = jnp.where(my_yh == 0, pair, other)
    odd = jnp.where(my_yh == 0, other, pair)
    received = lax.all_to_all(packed, ROW, 0, 0, tiled=True)
    column = jnp.stack([even[1], odd[1]])
    by_z = around(odd[0], "z")
    even = jnp.stack(around(even[0], "x"))
    even = jnp.stack(around(even, "z"))
    odd = jnp.stack(around(jnp.stack(by_z), "x"))

    data = received[:, : sources * share].reshape(rows, sources, share, BLOCK)
    label = received[:, sources * share : sources * share + sources, None, :]

    def belonging(half):
        wanted = (half * HALF + jnp.arange(HALF, dtype=jnp.int32)).astype(jnp.float32)
        return jnp.sum(
            jnp.where(label[None] == wanted[:, None, None, None, None], data[None], 0.0), axis=(1, 2)
        )

    start = belonging(my_yl) + rotated(belonging(1 - my_yl), "yl", 1)
    start = start + rotated(start, "core", 1)
    start = sum(around(start, "z"))

    goal = received[:, sources * share : sources * share + sources, 0].astype(jnp.int32)
    chosen = (goal[None] % cols) == jnp.arange(cols, dtype=jnp.int32)[:, None, None]
    outgoing = jnp.zeros((cols, rows, share, BLOCK), jnp.float32)
    for u in range(sources):
        outgoing = jnp.where(chosen[:, :, u, None, None], data[None, :, u], outgoing)
    slot_label = jnp.max(jnp.where(chosen, goal[None] // cols, -1), axis=2).astype(jnp.float32)
    slot_label = jnp.broadcast_to(slot_label[:, :, None], (cols, rows, BLOCK))
    outgoing = jnp.concatenate([outgoing.reshape(cols, BLOCK, BLOCK), slot_label], axis=1)

    even, odd, start = lax.optimization_barrier((even, odd, start))
    factors = (even, rotated(even, "core", 1), odd, rotated(odd, "core", 1))
    column, even = lax.optimization_barrier((column, even))
    coupling = jnp.stack(around(column, "x"))

    shape = (HALF, share, BLOCK)
    first = local_kernel(first_kernel, shape, place, start, *factors)
    passed = lax.ppermute(first, "yl", [(0, 1)])
    passed, outgoing = lax.optimization_barrier((passed, outgoing))
    residual = local_kernel(
        coupling_kernel, (share, BLOCK), place, start, passed, coupling
    )
    residual = jnp.stack(around(residual, "core"))
    upper, residual = lax.optimization_barrier((upper, residual))
    upper = with_layout_constraint(upper, Layout(major_to_minor=(0, 1, 2, 3)))
    factor = upper.transpose(0, 2, 1, 3)
    residual = jnp.stack(around(residual, "z"))
    copies = local_kernel(
        second_kernel, (HALF, 2, share, BLOCK), place, residual, first, *factors
    )
    panel_solution = lax.dynamic_index_in_dim(copies[:, 0], my_plane, 0, keepdims=False)

    own_rows = lax.all_to_all(
        copies.reshape(rows * 2, share, BLOCK), ROW + ("yl",), 0, 0, tiled=True
    ).reshape(rows, 2, share, BLOCK)
    a_keep, a_send, b_keep, *b_sends = update(place, own_rows, factor)
    outgoing, a_keep = lax.optimization_barrier((outgoing, a_keep))
    a_part = a_keep + rotated(a_send, "yh", 1)
    b_part = b_keep
    for step, b_send in zip((1, 2, 3), b_sends):
        b_part = b_part + rotated(b_send, "x", step)
    arrived = lax.all_to_all(outgoing, COL, 0, 0, tiled=True)
    b_part = b_part[0] + rotated(b_part[1], "yh", 1)
    a_part = a_part[0] + sum(rotated(a_part[step], "x", step) for step in (1, 2, 3))
    slot_of = arrived[:, BLOCK:, 0].astype(jnp.int32).reshape(cols * rows)
    held = pl.pallas_call(
        place_kernel,
        out_shape=jax.ShapeDtypeStruct((slots + 1, share, BLOCK), jnp.float32),
        in_specs=[SMEM, VMEM],
        out_specs=VMEM,
        cost_estimate=pl.CostEstimate(flops=100_000_000, bytes_accessed=2_000_000, transcendentals=0),
    )(slot_of, arrived)
    trailing = held[1:slots] + jnp.concatenate([a_part, b_part], axis=0)
    trailing = trailing.transpose(1, 0, 2)
    return panel_solution[:, None, None, :], trailing[:, :, None, :]


def solution(mesh):
    fine = Mesh(mesh.devices.reshape(4, 2, 2, 4, 2), ("x", "yh", "yl", "z", "core"))
    in_specs = (
        P(ROW, COL, None, None, None),
        P(ROW, COL, None),
        P(None, ROW, None, None, COL, None),
        P(None, COL, None, None),
    )
    out_specs = (P(ROW, None, COL, None), P(ROW, None, COL, None))
    return jax.shard_map(per_device, mesh=fine, in_specs=in_specs, out_specs=out_specs, check_vma=False)
```

```python
import jax
import jax.numpy as jnp
from jax import lax
from jax.experimental import pallas as pl
from jax.experimental.layout import Layout, with_layout_constraint
from jax.experimental.pallas import tpu as pltpu
from jax.sharding import Mesh
from jax.sharding import PartitionSpec as P


HIGHEST = lax.Precision.HIGHEST
ROW = ("x", "yh")
COL = ("yl", "z", "core")
PLANE = ("z", "core")
BLOCK = 128
HALF = 8
GRANT = 24 * 2**20
VMEM = pl.BlockSpec(memory_space=pltpu.VMEM)
SMEM = pl.BlockSpec(memory_space=pltpu.SMEM)


def rotated(array, axis, step):
    size = lax.axis_size(axis)
    return lax.ppermute(array, axis, [(i, (i + step) % size) for i in range(size)])


def around(array, axis):
    steps = range(1, lax.axis_size(axis))
    return [array] + [rotated(array, axis, step) for step in steps]


def split_bf16(value):
    high = value.astype(jnp.bfloat16)
    low = (value - high.astype(jnp.float32)).astype(jnp.bfloat16)
    return high, low


def product(left, right, right_dim=0):
    l_high, l_low = left
    r_high, r_low = split_bf16(right)
    dims = (((1,), (right_dim,)), ((), ()))
    both = jnp.concatenate([l_high, l_low], axis=0)
    first = lax.dot_general(both, r_high, dims, preferred_element_type=jnp.float32)
    second = lax.dot_general(l_high, r_low, dims, preferred_element_type=jnp.float32)
    rows = l_high.shape[0]
    return first[:rows] + first[rows:] + second


def solve_blocks(place_ref, start, even_refs, odd_refs):
    my_x, my_z, my_core = place_ref[0], place_ref[1], place_ref[2]

    def factor(j, i):
        dx = lax.rem(my_x - j // 2 + 4, 4)
        dz = lax.rem(my_z - i // 2 + 4, 4)
        own_ref, other_ref = even_refs if j % 2 == 0 else odd_refs
        at = (dz, dx) if j % 2 == 0 else (dx, dz)
        return jnp.where(my_core == i % 2, own_ref[at], other_ref[at])

    rest = [product(split_bf16(start(i)), factor(i, i), 1) for i in range(HALF)]
    for j in range(HALF):
        done = split_bf16(rest[j])
        for i in range(j + 1, HALF):
            rest[i] = rest[i] - product(done, factor(j, i))
    return rest


def first_kernel(place_ref, start_ref, e0_ref, e1_ref, o0_ref, o1_ref, out_ref):
    solved = solve_blocks(
        place_ref, lambda i: start_ref[i], (e0_ref, e1_ref), (o0_ref, o1_ref)
    )
    for i in range(HALF):
        out_ref[i] = solved[i]


def coupling_kernel(place_ref, start_ref, passed_ref, x_ref, out_ref):
    my_x, my_z, my_core = place_ref[0], place_ref[1], place_ref[2]
    left = jnp.concatenate([passed_ref[j] for j in range(HALF)], axis=1)
    right = [x_ref[lax.rem(my_x - j // 2 + 4, 4), j % 2] for j in range(HALF)]
    carried = product(split_bf16(left), jnp.concatenate(right, axis=0))
    out_ref[...] = start_ref[my_z * 2 + my_core] - carried


def second_kernel(place_ref, start_ref, first_ref, e0_ref, e1_ref, o0_ref, o1_ref, out_ref):
    my_z, my_core = place_ref[1], place_ref[2]

    def start(i):
        return start_ref[lax.rem(my_z - i // 2 + 4, 4), lax.rem(my_core + i, 2)]

    solved = solve_blocks(place_ref, start, (e0_ref, e1_ref), (o0_ref, o1_ref))
    for i in range(HALF):
        block = jnp.where(place_ref[3] == 0, first_ref[i], solved[i])
        out_ref[i, 0] = block
        out_ref[i, 1] = block


def update_kernel(
    place_ref, rows_ref, factor_ref,
    a_keep, a_send, b_keep, b_one, b_two, b_three, left_high, left_low,
):
    step = pl.program_id(0)
    count = factor_ref.shape[1]
    groups = [(yh, dx) for yh in range(2) for dx in range(4)]
    share = BLOCK // len(groups)

    @pl.when(step == 0)
    def _():
        for g, (yh, dx) in enumerate(groups):
            row = lax.rem(place_ref[0] + dx, 4) * 2 + lax.rem(place_ref[4] + yh, 2)
            for t in range(2):
                high, low = split_bf16(-rows_ref[row, t])
                at = (pl.ds(g * share, share), pl.ds(t * BLOCK, BLOCK))
                left_high[at] = high
                left_low[at] = low

    def fill(target):
        both = jnp.concatenate([left_high[...], left_low[...]], axis=0)
        for i in range(0, count, 2):
            halves = [
                jnp.concatenate([factor_ref[t, i], factor_ref[t, i + 1]], axis=1) for t in range(2)
            ]
            high, low = split_bf16(jnp.concatenate(halves, axis=0))
            first = jnp.dot(both, high, preferred_element_type=jnp.float32)
            second = jnp.dot(left_high[...], low, preferred_element_type=jnp.float32)
            total = first[:BLOCK] + first[BLOCK:] + second
            for k in range(2):
                for g, (yh, dx) in enumerate(groups):
                    target(i + k, yh, dx, total[g * share : (g + 1) * share, k * BLOCK : (k + 1) * BLOCK])

    def fill_a(slot, yh, dx, values):
        if slot > 0:
            (a_keep, a_send)[yh][dx, slot - 1] = values

    def fill_b(slot, yh, dx, values):
        (b_keep, b_one, b_two, b_three)[dx][yh, slot] = values

    pl.when(step == 0)(lambda: fill(fill_a))
    pl.when(step == 1)(lambda: fill(fill_b))


def pack_kernel(goal_ref, received_ref, out_ref):
    cols, share = out_ref.shape[0], 16
    sources = goal_ref.shape[0] // 8
    out_ref[:, :BLOCK] = jnp.zeros((cols, BLOCK, BLOCK), jnp.float32)
    out_ref[:, BLOCK:] = jnp.full((cols, 8, BLOCK), -1.0, jnp.float32)
    for r in range(8):
        for u in range(sources):
            goal = goal_ref[r * sources + u]
            col = lax.rem(goal, cols)
            slot = lax.div(goal, cols).astype(jnp.float32)
            out_ref[col, r * share : (r + 1) * share] = received_ref[r, u * share : (u + 1) * share]
            out_ref[col, BLOCK + r : BLOCK + r + 1] = jnp.full((1, BLOCK), slot, jnp.float32)


def place_kernel(slot_ref, arrived_ref, out_ref):
    spare = out_ref.shape[0] - 1
    share = out_ref.shape[1]
    for q in range(slot_ref.shape[0]):
        slot = slot_ref[q]
        rows = pl.ds(q % 8 * share, share)
        out_ref[jnp.where(slot < 0, spare, slot)] = arrived_ref[q // 8, rows, :]


def local_kernel(kernel, shape, *args):
    return pl.pallas_call(
        kernel,
        out_shape=jax.ShapeDtypeStruct(shape, jnp.float32),
        in_specs=[SMEM] + [VMEM] * (len(args) - 1),
        out_specs=VMEM,
        compiler_params=pltpu.CompilerParams(vmem_limit_bytes=GRANT),
        cost_estimate=pl.CostEstimate(flops=600_000_000, bytes_accessed=5_000_000, transcendentals=0),
    )(*args)


def update(place, own_rows, factor):
    slots, step = factor.shape[1], 16
    share = own_rows.shape[2]
    spec = pl.BlockSpec((2, step, BLOCK, BLOCK), lambda i: (0, i, 0, 0))
    shapes = [(4, 15, share, BLOCK)] * 2 + [(2, 16, share, BLOCK)] * 4
    return pl.pallas_call(
        update_kernel,
        out_shape=tuple(jax.ShapeDtypeStruct(shape, jnp.float32) for shape in shapes),
        grid=(slots // step,),
        in_specs=[SMEM, VMEM, spec],
        out_specs=(VMEM,) * 6,
        scratch_shapes=[pltpu.VMEM((BLOCK, 2 * BLOCK), jnp.bfloat16)] * 2,
        compiler_params=pltpu.CompilerParams(vmem_limit_bytes=GRANT),
        cost_estimate=pl.CostEstimate(flops=900_000_000, bytes_accessed=8_000_000, transcendentals=0),
    )(place, own_rows, factor)


def per_device(incoming, block_map, panel_row, diag_inverse):
    my_x, my_yh, my_yl, my_z, my_core = (lax.axis_index(a) for a in ("x", "yh", "yl", "z", "core"))
    my_row = lax.axis_index(ROW)
    my_plane = lax.axis_index(PLANE)
    rows, cols = lax.axis_size(ROW), lax.axis_size(COL)
    sources = incoming.shape[2]
    share = BLOCK // rows
    slots = panel_row.shape[3]
    place = jnp.stack([my_x, my_z, my_core, my_yl, my_yh]).astype(jnp.int32)

    targets = block_map.reshape(sources)
    blocks = incoming.reshape(sources, BLOCK, BLOCK)
    pieces = blocks.reshape(sources, rows, share, BLOCK).transpose(1, 0, 2, 3)
    labels = jnp.concatenate([targets, targets]).astype(jnp.float32)
    labels = jnp.broadcast_to(labels[None, :, None], (rows, 2 * sources, BLOCK))
    packed = jnp.concatenate([pieces.reshape(rows, sources * share, BLOCK), labels], axis=1)

    inverse = diag_inverse.reshape(BLOCK, BLOCK)
    upper = panel_row.reshape(2, BLOCK, slots, BLOCK)
    panel = lax.optimization_barrier(upper[:, :, 0, :])
    scaled = jnp.einsum("tpf,ef->tpe", panel, inverse, precision=HIGHEST)
    mine = jnp.where(my_yl == 0, scaled[0], scaled[1])
    mine = jnp.where(my_row == my_plane, inverse, mine)

    pair = jnp.stack([mine, panel[0]])
    other = lax.ppermute(pair, "yh", [(0, 1), (1, 0)])
    even = jnp.where(my_yh == 0, pair, other)
    odd = jnp.where(my_yh == 0, other, pair)
    received = lax.all_to_all(packed, ROW, 0, 0, tiled=True)
    column = jnp.stack([even[1], odd[1]])
    by_z = around(odd[0], "z")
    even = jnp.stack(around(even[0], "x"))
    even = jnp.stack(around(even, "z"))
    by_x = around(jnp.concatenate([jnp.stack(by_z), column]), "x")
    odd = jnp.stack([p[:4] for p in by_x])
    coupling = jnp.stack([p[4:] for p in by_x])

    data = received[:, : sources * share].reshape(rows, sources, share, BLOCK)
    label = received[:, sources * share : sources * share + sources, None, :]

    def belonging(half):
        wanted = (half * HALF + jnp.arange(HALF, dtype=jnp.int32)).astype(jnp.float32)
        return jnp.sum(
            jnp.where(label[None] == wanted[:, None, None, None, None], data[None], 0.0), axis=(1, 2)
        )

    start = belonging(my_yl) + rotated(belonging(1 - my_yl), "yl", 1)
    start = start + rotated(start, "core", 1)
    start = sum(around(start, "z"))

    goal = received[:, sources * share : sources * share + sources, 0].astype(jnp.int32)
    outgoing = local_kernel(
        pack_kernel, (cols, BLOCK + 8, BLOCK), goal.reshape(rows * sources), received
    )

    even, odd, start = lax.optimization_barrier((even, odd, start))
    factors = (even, rotated(even, "core", 1), odd, rotated(odd, "core", 1))

    shape = (HALF, share, BLOCK)
    first = local_kernel(first_kernel, shape, place, start, *factors)
    passed = lax.ppermute(first, "yl", [(0, 1)])
    passed, outgoing = lax.optimization_barrier((passed, outgoing))
    residual = local_kernel(
        coupling_kernel, (share, BLOCK), place, start, passed, coupling
    )
    residual = jnp.stack(around(residual, "core"))
    upper, residual = lax.optimization_barrier((upper, residual))
    upper = with_layout_constraint(upper, Layout(major_to_minor=(0, 1, 2, 3)))
    factor = upper.transpose(0, 2, 1, 3)
    residual = jnp.stack(around(residual, "z"))
    copies = local_kernel(second_kernel, (HALF, 2, share, BLOCK), place, residual, first, *factors)
    panel_solution = lax.dynamic_index_in_dim(copies[:, 0], my_plane, 0, keepdims=False)

    own_rows = lax.all_to_all(
        copies.reshape(rows * 2, share, BLOCK), ROW + ("yl",), 0, 0, tiled=True
    ).reshape(rows, 2, share, BLOCK)
    a_keep, a_send, b_keep, *b_sends = update(place, own_rows, factor)
    outgoing, a_keep = lax.optimization_barrier((outgoing, a_keep))
    a_part = a_keep + rotated(a_send, "yh", 1)
    b_part = b_keep
    for step, b_send in zip((1, 2, 3), b_sends):
        b_part = b_part + rotated(b_send, "x", step)
    arrived = lax.all_to_all(outgoing, COL, 0, 0, tiled=True)
    b_part = b_part[0] + rotated(b_part[1], "yh", 1)
    a_part = a_part[0] + sum(rotated(a_part[step], "x", step) for step in (1, 2, 3))
    slot_of = arrived[:, BLOCK:, 0].astype(jnp.int32).reshape(cols * rows)
    held = local_kernel(place_kernel, (slots + 1, share, BLOCK), slot_of, arrived)
    trailing = held[1:slots] + jnp.concatenate([a_part, b_part], axis=0)
    trailing = trailing.transpose(1, 0, 2)
    return panel_solution[:, None, None, :], trailing[:, :, None, :]


def solution(mesh):
    fine = Mesh(mesh.devices.reshape(4, 2, 2, 4, 2), ("x", "yh", "yl", "z", "core"))
    in_specs = (
        P(ROW, COL, None, None, None),
        P(ROW, COL, None),
        P(None, ROW, None, None, COL, None),
        P(None, COL, None, None),
    )
    out_specs = (P(ROW, None, COL, None), P(ROW, None, COL, None))
    return jax.shard_map(
        per_device, mesh=fine, in_specs=in_specs, out_specs=out_specs, check_vma=False
    )
```

```python
import jax
import jax.numpy as jnp
from jax import lax
from jax.experimental import pallas as pl
from jax.experimental.layout import Layout, with_layout_constraint
from jax.experimental.pallas import tpu as pltpu
from jax.sharding import Mesh
from jax.sharding import PartitionSpec as P


HIGHEST = lax.Precision.HIGHEST
ROW = ("x", "yh")
COL = ("yl", "z", "core")
PLANE = ("z", "core")
BLOCK = 128
HALF = 8
GRANT = 24 * 2**20
VMEM = pl.BlockSpec(memory_space=pltpu.VMEM)
SMEM = pl.BlockSpec(memory_space=pltpu.SMEM)


def rotated(array, axis, step):
    size = lax.axis_size(axis)
    return lax.ppermute(array, axis, [(i, (i + step) % size) for i in range(size)])


def around(array, axis):
    steps = range(1, lax.axis_size(axis))
    return [array] + [rotated(array, axis, step) for step in steps]


def split_bf16(value):
    high = value.astype(jnp.bfloat16)
    low = (value - high.astype(jnp.float32)).astype(jnp.bfloat16)
    return high, low


def product(left, right, right_dim=0):
    l_high, l_low = left
    r_high, r_low = split_bf16(right)
    dims = (((1,), (right_dim,)), ((), ()))
    both = jnp.concatenate([l_high, l_low], axis=0)
    first = lax.dot_general(both, r_high, dims, preferred_element_type=jnp.float32)
    second = lax.dot_general(l_high, r_low, dims, preferred_element_type=jnp.float32)
    rows = l_high.shape[0]
    return first[:rows] + first[rows:] + second


def solve_blocks(place_ref, start, even_refs, odd_refs):
    my_x, my_z, my_core = place_ref[0], place_ref[1], place_ref[2]

    def factor(j, i):
        dx = lax.rem(my_x - j // 2 + 4, 4)
        dz = lax.rem(my_z - i // 2 + 4, 4)
        own_ref, other_ref = even_refs if j % 2 == 0 else odd_refs
        at = (dz, dx) if j % 2 == 0 else (dx, dz)
        return jnp.where(my_core == i % 2, own_ref[at], other_ref[at])

    rest = [product(split_bf16(start(i)), factor(i, i), 1) for i in range(HALF)]
    for j in range(HALF):
        done = split_bf16(rest[j])
        for i in range(j + 1, HALF):
            rest[i] = rest[i] - product(done, factor(j, i))
    return rest


def first_kernel(place_ref, start_ref, e0_ref, e1_ref, o0_ref, o1_ref, out_ref):
    solved = solve_blocks(
        place_ref, lambda i: start_ref[i], (e0_ref, e1_ref), (o0_ref, o1_ref)
    )
    for i in range(HALF):
        out_ref[i] = solved[i]


def coupling_kernel(place_ref, start_ref, passed_ref, x_ref, out_ref):
    my_x, my_z, my_core = place_ref[0], place_ref[1], place_ref[2]
    left = jnp.concatenate([passed_ref[j] for j in range(HALF)], axis=1)
    right = [x_ref[lax.rem(my_x - j // 2 + 4, 4), j % 2] for j in range(HALF)]
    carried = product(split_bf16(left), jnp.concatenate(right, axis=0))
    out_ref[...] = start_ref[my_z * 2 + my_core] - carried


def second_kernel(place_ref, start_ref, first_ref, e0_ref, e1_ref, o0_ref, o1_ref, out_ref):
    my_z, my_core = place_ref[1], place_ref[2]

    def start(i):
        return start_ref[lax.rem(my_z - i // 2 + 4, 4), lax.rem(my_core + i, 2)]

    solved = solve_blocks(place_ref, start, (e0_ref, e1_ref), (o0_ref, o1_ref))
    for i in range(HALF):
        block = jnp.where(place_ref[3] == 0, first_ref[i], solved[i])
        out_ref[i, 0] = block
        out_ref[i, 1] = block


def update_kernel(
    place_ref, rows_ref, factor_ref,
    a_keep, a_send, b_keep, b_one, b_two, b_three, left_high, left_low,
):
    step = pl.program_id(0)
    count = factor_ref.shape[1]
    groups = [(yh, dx) for yh in range(2) for dx in range(4)]
    share = BLOCK // len(groups)

    @pl.when(step == 0)
    def _():
        for g, (yh, dx) in enumerate(groups):
            row = lax.rem(place_ref[0] + dx, 4) * 2 + lax.rem(place_ref[4] + yh, 2)
            for t in range(2):
                high, low = split_bf16(-rows_ref[row, t])
                at = (pl.ds(g * share, share), pl.ds(t * BLOCK, BLOCK))
                left_high[at] = high
                left_low[at] = low

    def fill(target):
        both = jnp.concatenate([left_high[...], left_low[...]], axis=0)
        for i in range(0, count, 2):
            halves = [
                jnp.concatenate([factor_ref[t, i], factor_ref[t, i + 1]], axis=1) for t in range(2)
            ]
            high, low = split_bf16(jnp.concatenate(halves, axis=0))
            first = jnp.dot(both, high, preferred_element_type=jnp.float32)
            second = jnp.dot(left_high[...], low, preferred_element_type=jnp.float32)
            total = first[:BLOCK] + first[BLOCK:] + second
            for k in range(2):
                for g, (yh, dx) in enumerate(groups):
                    target(i + k, yh, dx, total[g * share : (g + 1) * share, k * BLOCK : (k + 1) * BLOCK])

    def fill_a(slot, yh, dx, values):
        if slot > 0:
            (a_keep, a_send)[yh][dx, slot - 1] = values

    def fill_b(slot, yh, dx, values):
        (b_keep, b_one, b_two, b_three)[dx][yh, slot] = values

    pl.when(step == 0)(lambda: fill(fill_a))
    pl.when(step == 1)(lambda: fill(fill_b))


def pack_kernel(goal_ref, received_ref, out_ref):
    cols, share = out_ref.shape[0], 16
    sources = goal_ref.shape[0] // 8
    out_ref[:, :BLOCK] = jnp.zeros((cols, BLOCK, BLOCK), jnp.float32)
    out_ref[:, BLOCK:] = jnp.full((cols, 8, BLOCK), -1.0, jnp.float32)
    for r in range(8):
        for u in range(sources):
            goal = goal_ref[r * sources + u]
            col = lax.rem(goal, cols)
            slot = lax.div(goal, cols).astype(jnp.float32)
            out_ref[col, r * share : (r + 1) * share] = received_ref[r, u * share : (u + 1) * share]
            out_ref[col, BLOCK + r : BLOCK + r + 1] = jnp.full((1, BLOCK), slot, jnp.float32)


def place_kernel(slot_ref, arrived_ref, out_ref):
    spare = out_ref.shape[0] - 1
    share = out_ref.shape[1]
    for q in range(slot_ref.shape[0]):
        slot = slot_ref[q]
        rows = pl.ds(q % 8 * share, share)
        out_ref[jnp.where(slot < 0, spare, slot)] = arrived_ref[q // 8, rows, :]


def local_kernel(kernel, shape, *args):
    return pl.pallas_call(
        kernel,
        out_shape=jax.ShapeDtypeStruct(shape, jnp.float32),
        in_specs=[SMEM] + [VMEM] * (len(args) - 1),
        out_specs=VMEM,
        compiler_params=pltpu.CompilerParams(vmem_limit_bytes=GRANT),
        cost_estimate=pl.CostEstimate(flops=600_000_000, bytes_accessed=5_000_000, transcendentals=0),
    )(*args)


def update(place, own_rows, factor):
    slots, step = factor.shape[1], 16
    share = own_rows.shape[2]
    spec = pl.BlockSpec((2, step, BLOCK, BLOCK), lambda i: (0, i, 0, 0))
    shapes = [(4, 15, share, BLOCK)] * 2 + [(2, 16, share, BLOCK)] * 4
    return pl.pallas_call(
        update_kernel,
        out_shape=tuple(jax.ShapeDtypeStruct(shape, jnp.float32) for shape in shapes),
        grid=(slots // step,),
        in_specs=[SMEM, VMEM, spec],
        out_specs=(VMEM,) * 6,
        scratch_shapes=[pltpu.VMEM((BLOCK, 2 * BLOCK), jnp.bfloat16)] * 2,
        compiler_params=pltpu.CompilerParams(vmem_limit_bytes=GRANT),
        cost_estimate=pl.CostEstimate(flops=900_000_000, bytes_accessed=8_000_000, transcendentals=0),
    )(place, own_rows, factor)


def per_device(incoming, block_map, panel_row, diag_inverse):
    my_x, my_yh, my_yl, my_z, my_core = (lax.axis_index(a) for a in ("x", "yh", "yl", "z", "core"))
    my_row = lax.axis_index(ROW)
    my_plane = lax.axis_index(PLANE)
    rows, cols = lax.axis_size(ROW), lax.axis_size(COL)
    sources = incoming.shape[2]
    share = BLOCK // rows
    slots = panel_row.shape[3]
    place = jnp.stack([my_x, my_z, my_core, my_yl, my_yh]).astype(jnp.int32)

    targets = block_map.reshape(sources)
    blocks = incoming.reshape(sources, BLOCK, BLOCK)
    pieces = blocks.reshape(sources, rows, share, BLOCK).transpose(1, 0, 2, 3)
    labels = jnp.concatenate([targets, targets]).astype(jnp.float32)
    labels = jnp.broadcast_to(labels[None, :, None], (rows, 2 * sources, BLOCK))
    packed = jnp.concatenate([pieces.reshape(rows, sources * share, BLOCK), labels], axis=1)

    inverse = diag_inverse.reshape(BLOCK, BLOCK)
    upper = panel_row.reshape(2, BLOCK, slots, BLOCK)
    panel = lax.optimization_barrier(upper[:, :, 0, :])
    scaled = jnp.einsum("tpf,ef->tpe", panel, inverse, precision=HIGHEST)
    mine = jnp.where(my_yl == 0, scaled[0], scaled[1])
    mine = jnp.where(my_row == my_plane, inverse, mine)

    pair = jnp.stack([mine, panel[0]])
    other = lax.ppermute(pair, "yh", [(0, 1), (1, 0)])
    even = jnp.where(my_yh == 0, pair, other)
    odd = jnp.where(my_yh == 0, other, pair)
    received = lax.all_to_all(packed, ROW, 0, 0, tiled=True)
    column = jnp.stack([even[1], odd[1]])
    by_z = around(odd[0], "z")
    even = jnp.stack(around(even[0], "x"))
    even = jnp.stack(around(even, "z"))
    odd = jnp.stack(around(jnp.stack(by_z), "x"))

    data = received[:, : sources * share].reshape(rows, sources, share, BLOCK)
    label = received[:, sources * share : sources * share + sources, None, :]

    def belonging(half):
        wanted = (half * HALF + jnp.arange(HALF, dtype=jnp.int32)).astype(jnp.float32)
        return jnp.sum(
            jnp.where(label[None] == wanted[:, None, None, None, None], data[None], 0.0), axis=(1, 2)
        )

    start = belonging(my_yl) + rotated(belonging(1 - my_yl), "yl", 1)
    start = start + rotated(start, "core", 1)
    start = sum(around(start, "z"))

    goal = received[:, sources * share : sources * share + sources, 0].astype(jnp.int32)
    outgoing = local_kernel(
        pack_kernel, (cols, BLOCK + 8, BLOCK), goal.reshape(rows * sources), received
    )

    even, odd, start = lax.optimization_barrier((even, odd, start))
    factors = (even, rotated(even, "core", 1), odd, rotated(odd, "core", 1))
    coupling = jnp.stack(around(column, "x"))

    shape = (HALF, share, BLOCK)
    first = local_kernel(first_kernel, shape, place, start, *factors)
    passed = lax.ppermute(first, "yl", [(0, 1)])
    passed, outgoing = lax.optimization_barrier((passed, outgoing))
    residual = local_kernel(
        coupling_kernel, (share, BLOCK), place, start, passed, coupling
    )
    residual = jnp.stack(around(residual, "core"))
    upper, residual = lax.optimization_barrier((upper, residual))
    upper = with_layout_constraint(upper, Layout(major_to_minor=(0, 1, 2, 3)))
    factor = upper.transpose(0, 2, 1, 3)
    residual = jnp.stack(around(residual, "z"))
    copies = local_kernel(second_kernel, (HALF, 2, share, BLOCK), place, residual, first, *factors)
    panel_solution = lax.dynamic_index_in_dim(copies[:, 0], my_plane, 0, keepdims=False)

    own_rows = lax.all_to_all(
        copies.reshape(rows * 2, share, BLOCK), ROW + ("yl",), 0, 0, tiled=True
    ).reshape(rows, 2, share, BLOCK)
    a_keep, a_send, b_keep, *b_sends = update(place, own_rows, factor)
    outgoing, a_keep = lax.optimization_barrier((outgoing, a_keep))
    a_part = a_keep + rotated(a_send, "yh", 1)
    b_part = b_keep
    for step, b_send in zip((1, 2, 3), b_sends):
        b_part = b_part + rotated(b_send, "x", step)
    arrived = lax.all_to_all(outgoing, COL, 0, 0, tiled=True)
    b_part = b_part[0] + rotated(b_part[1], "yh", 1)
    a_part = a_part[0] + sum(rotated(a_part[step], "x", step) for step in (1, 2, 3))
    slot_of = arrived[:, BLOCK:, 0].astype(jnp.int32).reshape(cols * rows)
    held = local_kernel(place_kernel, (slots + 1, share, BLOCK), slot_of, arrived)
    trailing = held[1:slots] + jnp.concatenate([a_part, b_part], axis=0)
    trailing = trailing.transpose(1, 0, 2)
    return panel_solution[:, None, None, :], trailing[:, :, None, :]


def solution(mesh):
    fine = Mesh(mesh.devices.reshape(4, 2, 2, 4, 2), ("x", "yh", "yl", "z", "core"))
    in_specs = (
        P(ROW, COL, None, None, None),
        P(ROW, COL, None),
        P(None, ROW, None, None, COL, None),
        P(None, COL, None, None),
    )
    out_specs = (P(ROW, None, COL, None), P(ROW, None, COL, None))
    return jax.shard_map(
        per_device, mesh=fine, in_specs=in_specs, out_specs=out_specs, check_vma=False
    )
```
